32 devices in a mesh: dp: 8 (over y, x, core), tensor: 4 (over z).
Axes of the slice: x: 2, y: 2, z: 4, core: 2. Of those that a mesh axis runs over, the one named last changes fastest.
Arguments:
- tokens: bfloat16 [8192, 2048], P('dp'), may hold values from -6 to 6
- attn_norm_gain: float32 [2048], replicated, may hold values from 0.5 to 1.5
- attn_norm_bias: float32 [2048], replicated, may hold values from -1.8 to 1.8
- mlp_norm_gain: float32 [2048], replicated, may hold values from 0.5 to 1.5
- mlp_norm_bias: float32 [2048], replicated, may hold values from -1.8 to 1.8
- w_qkv: bfloat16 [2048, 6144], P(None, 'tensor'), may hold values from -0.125 to 0.125
- qkv_bias: float32 [6144], P('tensor'), may hold values from -3 to 3
- w_out: bfloat16 [2048, 2048], P('tensor'), may hold values from -0.75 to 0.75
- w_up: bfloat16 [2048, 8192], P(None, 'tensor'), may hold values from -0.125 to 0.125
- up_bias: float32 [8192], P('tensor'), may hold values from -3 to 3
- w_down: bfloat16 [8192, 2048], P('tensor'), may hold values from -0.0625 to 0.0625
- out_bias: float32 [2048], replicated, may hold values from -3 to 3
- cotangent: bfloat16 [8192, 2048], P('dp'), may hold values from -6 to 6
Outputs:
- block_out: bfloat16 [8192, 2048], P('dp')
- input_grad: float32 [8192, 2048], P('dp')
- grad_w_qkv: float32 [2048, 6144], P('dp', 'tensor')
- grad_w_out: float32 [2048, 2048], P('tensor', 'dp')
- grad_w_up: float32 [2048, 8192], P('dp', 'tensor')
- grad_w_down: float32 [8192, 2048], P('tensor', 'dp')
- grad_norm_params: float32 [4, 2048], replicated
- grad_qkv_bias: float32 [6144], replicated
- grad_up_bias: float32 [8192], replicated
- grad_out_bias: float32 [2048], replicated
The draws below stay inside these ranges and needn't reach their ends.
All inputs are finite; a program needn't handle non-finite values.
Results may differ from the reference program's by a relative error of at most 0.012.
Values may be sent and summed in bfloat16 or wider, within the bound.
A program may use at most 192 MiB of HBM per device.

```python
import jax
import jax.numpy as jnp
from jax import lax

D = 2048
H = 8
HD = 256
FF = 8192
ROT = 64
SEQ_LEN = 1024
TOKENS = 8192


def block_scale(own_key, shape, shards, smallest, high):
    def one(axis_at, blocks):
        steps = jax.random.uniform(jax.random.fold_in(jax.random.fold_in(own_key, 6), axis_at), (blocks,), jnp.float32, smallest / len(shards), high / len(shards))
        return jnp.repeat(jnp.exp(steps), shape[axis_at] // blocks).reshape((-1,) + (1,) * (len(shape) - axis_at - 1))

    factor_of = one(*shards[0])
    for cut in shards[1:]:
        factor_of = factor_of * one(*cut)
    return factor_of


def gaussian(stream_key, shape, width, reach, shards=(), kind=jnp.bfloat16):
    array = jax.random.normal(stream_key, shape, jnp.float32) * width
    if len(shards) > 0:
        array = block_scale(stream_key, shape, shards, -0.22, 0.18) * array
    return jnp.clip(array, min=-reach, max=reach).astype(kind)


def setup_inputs(seed: int = 0) -> dict:
    streams_of = jax.random.split(jax.random.key(seed), 14)
    return {
        "tokens": gaussian(streams_of[0], (TOKENS, D), 1.0, 6.0, ((0, 8),)),
        "attn_norm_gain": jnp.clip(1.0 + 0.1 * jax.random.normal(streams_of[1], (D,), jnp.float32), 0.5, 1.5),
        "attn_norm_bias": gaussian(streams_of[2], (D,), 0.3, 1.8, (), jnp.float32),
        "mlp_norm_gain": jnp.clip(1.0 + 0.1 * jax.random.normal(streams_of[3], (D,), jnp.float32), 0.5, 1.5),
        "mlp_norm_bias": gaussian(streams_of[4], (D,), 0.3, 1.8, (), jnp.float32),
        "w_qkv": gaussian(streams_of[5], (D, 3 * H * HD), D ** -0.5, 0.125, ((1, 4),)),
        "qkv_bias": gaussian(streams_of[6], (3 * H * HD,), 0.5, 3.0, ((0, 4),), jnp.float32),
        "w_out": gaussian(streams_of[7], (H * HD, D), (H * HD // 32) ** -0.5, 0.75, ((0, 4),)),
        "w_up": gaussian(streams_of[8], (D, FF), D ** -0.5, 0.125, ((1, 4),)),
        "up_bias": gaussian(streams_of[9], (FF,), 0.5, 3.0, ((0, 4),), jnp.float32),
        "w_down": gaussian(streams_of[10], (FF, D), FF ** -0.5, 0.0625, ((0, 4),)),
        "out_bias": gaussian(streams_of[11], (D,), 0.5, 3.0, (), jnp.float32),
        "cotangent": gaussian(streams_of[12], (TOKENS, D), 1.0, 6.0, ((0, 8),)),
    }


EPSILON = 1e-05
ROPE_BASE = 10000.0
MASKED = -1e+30

@jax.custom_vjp
def low(v):
    return lax.optimization_barrier(v.astype(jnp.bfloat16)).astype(jnp.float32)

@jax.custom_vjp
def low_back(v):
    return v

def low_keep(v):
    return (low(v), None)

def low_pass(kept, grad):
    return (grad,)

def back_keep(v):
    return (v, None)

def back_low(kept, grad):
    return (low(grad),)
low.defvjp(low_keep, low_pass)
low_back.defvjp(back_keep, back_low)

def precise(left, right):
    return jnp.dot(left, right, preferred_element_type=jnp.float32, precision=lax.Precision.HIGHEST)

def normalize(rows_in, norm_gain, norm_bias):
    row_mean = lax.optimization_barrier(jnp.mean(rows_in, axis=1, keepdims=True))
    centred = rows_in - row_mean
    variance = lax.optimization_barrier(jnp.mean(centred * centred, axis=1, keepdims=True))
    return centred * lax.rsqrt(variance + EPSILON) * norm_gain + norm_bias

def rotary_tables(length):
    half_rot = ROT // 2
    freqs = ROPE_BASE ** (-(2.0 * jnp.arange(half_rot, dtype=jnp.float32)) / ROT)
    angles = jnp.arange(length, dtype=jnp.float32)[:, None] * freqs[None, :]
    return (jnp.cos(angles), jnp.sin(angles))

def rotate(values, cosine_table, sine_table):
    half_rot = ROT // 2
    first_half = values[..., :half_rot]
    second_half = values[..., half_rot:ROT]
    cos_rows = cosine_table[:, None, :]
    sin_rows = sine_table[:, None, :]
    return jnp.concatenate([first_half * cos_rows - second_half * sin_rows, second_half * cos_rows + first_half * sin_rows, values[..., ROT:]], axis=-1)

def block_forward(params, rows_in):
    attn_gain, attn_shift, mlp_gain, mlp_shift, weight_qkv, bias_qkv, weight_out, weight_up, bias_up, weight_down, bias_out = params
    length = rows_in.shape[0]
    attn_in = low(normalize(rows_in, attn_gain, attn_shift))
    mlp_in = low(normalize(rows_in, mlp_gain, mlp_shift))
    projected = low_back(precise(attn_in, weight_qkv) + bias_qkv).reshape(length, H, 3, HD)
    cosine_table, sine_table = rotary_tables(length)
    queries = low(rotate(projected[:, :, 0], cosine_table, sine_table))
    keys_all = low(rotate(projected[:, :, 1], cosine_table, sine_table))
    values_all = low(projected[:, :, 2])
    scaling = float(HD) ** (-0.5)
    scores = low_back(jnp.einsum('qhd,khd->hqk', queries, keys_all, precision=lax.Precision.HIGHEST) * scaling)
    positions = jnp.arange(length)
    causal = positions[None, :] <= positions[:, None]
    probs = jax.nn.softmax(jnp.where(causal[None], scores, MASKED), axis=-1)
    attended = jnp.einsum('hqk,khd->qhd', low(probs), values_all, precision=lax.Precision.HIGHEST)
    attended = low_back(low(attended)).reshape(length, H * HD)
    attn_branch = precise(attended, weight_out)
    hidden = low(jax.nn.gelu(low_back(precise(mlp_in, weight_up) + bias_up), approximate=False))
    mlp_branch = precise(hidden, weight_down)
    return rows_in + attn_branch + mlp_branch + bias_out

def reference(tokens, attn_norm_gain, attn_norm_bias, mlp_norm_gain, mlp_norm_bias, w_qkv, qkv_bias, w_out, w_up, up_bias, w_down, out_bias, cotangent):
    params = tuple((member.astype(jnp.float32) for member in (attn_norm_gain, attn_norm_bias, mlp_norm_gain, mlp_norm_bias, w_qkv, qkv_bias, w_out, w_up, up_bias, w_down, out_bias)))
    seq_total = TOKENS // SEQ_LEN
    inputs = tokens.astype(jnp.float32).reshape(seq_total, SEQ_LEN, D)
    seeds = cotangent.astype(jnp.float32).reshape(seq_total, SEQ_LEN, D)
    totals = jax.tree.map(jnp.zeros_like, params)

    def one_sequence(carried, seq_pair):
        rows_in, rows_grad = seq_pair
        result, pullback = jax.vjp(block_forward, params, rows_in)
        param_grads, rows_back = pullback(rows_grad)
        return (jax.tree.map(jnp.add, carried, param_grads), (result, rows_back))
    totals, (results, input_grads) = lax.scan(one_sequence, totals, (inputs, seeds))
    grad_attn_gain, grad_attn_shift, grad_mlp_gain, grad_mlp_shift, grad_w_qkv, grad_qkv_bias, grad_w_out, grad_w_up, grad_up_bias, grad_w_down, grad_out_bias = totals
    grad_norm_params = jnp.stack([grad_attn_gain, grad_attn_shift, grad_mlp_gain, grad_mlp_shift])
    block_out = results.reshape(TOKENS, D).astype(jnp.bfloat16)
    input_grad = input_grads.reshape(TOKENS, D)
    return (block_out, input_grad, grad_w_qkv, grad_w_out, grad_w_up, grad_w_down, grad_norm_params, grad_qkv_bias, grad_up_bias, grad_out_bias)
```

```python
import functools

import jax
import jax.numpy as jnp
from jax import lax
from jax.experimental import pallas as pl
from jax.experimental.pallas import tpu as pltpu
from jax.sharding import PartitionSpec as P

HD = 256
ROT = 64
SEQ_LEN = 1024
EPSILON = 1e-05
ROPE_BASE = 10000.0
MASKED = -1e30
BF = jnp.bfloat16
F32 = jnp.float32
VMEM_LIMIT = 56 * 1024 * 1024
B_ROWS = (256, 256, 256, 256)
N_ROWS = (256, 256, 256, 128, 128)

NN = (((1,), (0,)), ((), ()))
NT = (((1,), (1,)), ((), ()))
TN = (((0,), (0,)), ((), ()))


def dot(a, b, dims=NN):
    return lax.dot_general(a, b, dims, preferred_element_type=F32)


def call(body, name, grid, in_specs, out_specs, out_shape, flops, scratch=()):
    moved = sum(int(s.size) * s.dtype.itemsize for s in out_shape)
    return pl.pallas_call(
        body,
        name=name,
        grid=grid,
        in_specs=in_specs,
        out_specs=out_specs,
        out_shape=out_shape,
        scratch_shapes=list(scratch),
        compiler_params=pltpu.CompilerParams(vmem_limit_bytes=VMEM_LIMIT),
        cost_estimate=pl.CostEstimate(flops=flops, bytes_accessed=3 * moved, transcendentals=0),
    )


def shape(dims, dtype):
    return jax.ShapeDtypeStruct(dims, dtype)


def norm_body(tok, ga, ba, gm, bm, attn_in, mlp_in, mean_out, inv_out):
    t = tok[...].astype(F32)
    mean = jnp.mean(t, axis=1, keepdims=True)
    centred = t - mean
    inv = lax.rsqrt(jnp.mean(centred * centred, axis=1, keepdims=True) + EPSILON)
    normed = centred * inv
    attn_in[...] = (normed * ga[...] + ba[...]).astype(BF)
    mlp_in[...] = (normed * gm[...] + bm[...]).astype(BF)
    mean_out[...] = jnp.broadcast_to(mean, mean_out.shape)
    inv_out[...] = jnp.broadcast_to(inv, inv_out.shape)


def norm_forward(tokens, ga, ba, gm, bm):
    rows, width = tokens.shape
    block = 128
    row = pl.BlockSpec((block, width), lambda i: (i, 0))
    vec = pl.BlockSpec((1, width), lambda i: (0, 0))
    stat = pl.BlockSpec((block, 128), lambda i: (i, 0))
    return call(
        norm_body, "norm_forward", (rows // block,),
        [row, vec, vec, vec, vec], [row, row, stat, stat],
        [shape((rows, width), BF)] * 2 + [shape((rows, 128), F32)] * 2,
        10 * rows * width,
    )(tokens, ga[None], ba[None], gm[None], bm[None])


def turn(values, cosines, sines):
    low = values[:, :128]
    lane = lax.broadcasted_iota(jnp.int32, low.shape, 1)
    partner = jnp.where(
        lane < ROT // 2, pltpu.roll(low, 128 - ROT // 2, 1), pltpu.roll(low, ROT // 2, 1)
    )
    return jnp.concatenate([low * cosines + partner * sines, values[:, 128:]], axis=1)


def attention_body(block, proj, grad, cosines, sines, attended, proj_grad, bias_grad, qs, ks, vs, dk, dv):
    length = proj.shape[0]
    scaling = float(HD) ** (-0.5)
    qs[...] = turn(proj[:, :HD], cosines[...], sines[...]).astype(BF)
    ks[...] = turn(proj[:, HD : 2 * HD], cosines[...], sines[...]).astype(BF)
    vs[...] = proj[:, 2 * HD :].astype(BF)
    dk[...] = jnp.zeros_like(dk)
    dv[...] = jnp.zeros_like(dv)
    q_bias = jnp.zeros((1, HD), F32)
    for start in range(0, length, block):
        here = pl.ds(start, block)
        stop = start + block
        q = qs[here, :]
        g = grad[here, :]
        k = ks[:stop, :]
        v = vs[:stop, :]
        scores = dot(q, k, NT) * scaling
        rows_at = lax.broadcasted_iota(jnp.int32, scores.shape, 0) + start
        keys_at = lax.broadcasted_iota(jnp.int32, scores.shape, 1)
        scores = jnp.where(keys_at <= rows_at, scores, MASKED)
        top = jnp.max(scores, axis=1, keepdims=True)
        raised = jnp.exp(scores - top)
        probs = raised / jnp.sum(raised, axis=1, keepdims=True)
        probs_low = probs.astype(BF)
        attended[here, :] = dot(probs_low, v).astype(BF)
        prob_grad = dot(g, v, NT)
        row_dot = jnp.sum(probs * prob_grad, axis=1, keepdims=True)
        score_grad = (probs * (prob_grad - row_dot)).astype(BF)
        dq = turn(dot(score_grad, k) * scaling, cosines[here, :], -sines[here, :]).astype(BF)
        proj_grad[here, :HD] = dq
        q_bias = q_bias + jnp.sum(dq.astype(F32), axis=0, keepdims=True)
        dk[:stop, :] += dot(score_grad, q, TN)
        dv[:stop, :] += dot(probs_low, g, TN)
    k_low = turn(dk[...] * scaling, cosines[...], -sines[...]).astype(BF)
    v_low = dv[...].astype(BF)
    proj_grad[:, HD : 2 * HD] = k_low
    proj_grad[:, 2 * HD :] = v_low
    sums = [q_bias, jnp.sum(k_low.astype(F32), axis=0, keepdims=True), jnp.sum(v_low.astype(F32), axis=0, keepdims=True)]
    bias_grad[...] = jnp.concatenate(sums, axis=1)


def attention(projected, grad, cosines, sines):
    rows, width = projected.shape
    heads = width // (3 * HD)
    seqs = rows // SEQ_LEN
    block = 256
    tri = pl.BlockSpec((SEQ_LEN, 3 * HD), lambda s, h: (s, h))
    one = pl.BlockSpec((SEQ_LEN, HD), lambda s, h: (s, h))
    table = pl.BlockSpec((SEQ_LEN, 128), lambda s, h: (0, 0))
    bias = pl.BlockSpec((None, 1, 3 * HD), lambda s, h: (s, 0, h))
    half = [pltpu.VMEM((SEQ_LEN, HD), BF)] * 3 + [pltpu.VMEM((SEQ_LEN, HD), F32)] * 2
    attended, proj_grad, bias_grad = call(
        functools.partial(attention_body, block), "attention", (seqs, heads),
        [tri, one, table, table], [one, tri, bias],
        [shape((rows, heads * HD), BF), shape((rows, width), BF), shape((seqs, 1, width), F32)],
        8 * rows * SEQ_LEN * HD * heads, half,
    )(projected, grad, cosines, sines)
    return attended, proj_grad, jnp.sum(bias_grad, axis=(0, 1))


def rotary_tables(length):
    half = ROT // 2
    freqs = ROPE_BASE ** (-(2.0 * jnp.arange(half, dtype=F32)) / ROT)
    angles = jnp.arange(length, dtype=F32)[:, None] * freqs[None, :]
    cosine, sine = jnp.cos(angles), jnp.sin(angles)
    rest = (length, 128 - ROT)
    return (
        jnp.concatenate([cosine, cosine, jnp.ones(rest, F32)], axis=1),
        jnp.concatenate([-sine, sine, jnp.zeros(rest, F32)], axis=1),
    )


def middle_body(x, cot, w_up, bias, w_down, hidden, up_grad, sums):
    u = dot(x[...], w_up[...]) + bias[...]
    hg = dot(cot[...], w_down[...], NT)
    cdf = 0.5 * (1.0 + lax.erf(u * (0.5**0.5)))
    pdf = jnp.exp(-0.5 * u * u) * 0.3989422804014327
    hidden[...] = (u * cdf).astype(BF)
    ug = (hg * (cdf + u * pdf)).astype(BF)
    up_grad[...] = ug
    sums[...] = jnp.sum(ug.astype(F32), axis=0, keepdims=True)


def middle(x, cot, w_up, up_bias, w_down, at, rows):
    width, ff = w_up.shape
    tile = 256
    i = at // rows
    row = pl.BlockSpec((rows, width), lambda j: (i, 0))
    col = pl.BlockSpec((rows, tile), lambda j: (0, j))
    vec = pl.BlockSpec((1, tile), lambda j: (0, j))
    return call(
        middle_body, "middle", (ff // tile,),
        [row, row, pl.BlockSpec((width, tile), lambda j: (0, j)), vec, pl.BlockSpec((tile, width), lambda j: (j, 0))],
        [col, col, vec],
        [shape((rows, ff), BF), shape((rows, ff), BF), shape((1, ff), F32)],
        4 * rows * width * ff,
    )(x, cot, w_up, up_bias[None], w_down)


def branch_body(hidden, attended, w_down, w_out, out):
    out[...] = (dot(hidden[...], w_down[...]) + dot(attended[...], w_out[...])).astype(BF)


def branch(hidden, h_at, attended, a_at, w_down, w_out, rows):
    ff, width = w_down.shape
    own = w_out.shape[0]
    tile = 256
    hi, ai = h_at // rows, a_at // rows
    return call(
        branch_body, "branch", (width // tile,),
        [
            pl.BlockSpec((rows, ff), lambda j: (hi, 0)),
            pl.BlockSpec((rows, own), lambda j: (ai, 0)),
            pl.BlockSpec((ff, tile), lambda j: (0, j)),
            pl.BlockSpec((own, tile), lambda j: (0, j)),
        ],
        [pl.BlockSpec((rows, tile), lambda j: (0, j))],
        [shape((rows, width), BF)],
        2 * rows * width * (ff + own),
    )(hidden, attended, w_down, w_out)[0]


def back_body(ug, pg, w_up, w_qkv, tok, mean, inv, ga, gm, out, sums):
    m = dot(ug[...], w_up[...], NT)
    a = dot(pg[...], w_qkv[...], NT)
    normed = (tok[...].astype(F32) - mean[:, :1]) * inv[:, :1]
    out[...] = (a * ga[...] + m * gm[...]).astype(BF)
    total = lambda v: jnp.sum(v, axis=0, keepdims=True)
    sums[...] = jnp.concatenate([total(a * normed), total(a), total(m * normed), total(m)], axis=0)


def back(ug, u_at, pg, p_at, w_up, w_qkv, tokens, mean, inv, ga, gm, rows):
    width, ff = w_up.shape
    own = w_qkv.shape[1]
    tile = 256
    ui, pi = u_at // rows, p_at // rows
    vec = pl.BlockSpec((1, tile), lambda j: (0, j))
    stat = pl.BlockSpec((rows, 128), lambda j: (pi, 0))
    return call(
        back_body, "back", (width // tile,),
        [
            pl.BlockSpec((rows, ff), lambda j: (ui, 0)),
            pl.BlockSpec((rows, own), lambda j: (pi, 0)),
            pl.BlockSpec((tile, ff), lambda j: (j, 0)),
            pl.BlockSpec((tile, own), lambda j: (j, 0)),
            pl.BlockSpec((rows, tile), lambda j: (pi, j)),
            stat, stat, vec, vec,
        ],
        [pl.BlockSpec((rows, tile), lambda j: (0, j)), pl.BlockSpec((4, tile), lambda j: (0, j))],
        [shape((rows, width), BF), shape((4, width), F32)],
        2 * rows * width * (ff + own),
    )(ug, pg, w_up, w_qkv, tokens, mean, inv, ga[None], gm[None])


def line_sum(part, finish):
    d = lax.axis_index("tensor")
    inner = (d == 1) | (d == 2)
    got = lax.ppermute(part, "tensor", [(0, 1), (3, 2)])
    mine = (part.astype(F32) + got.astype(F32)).astype(BF)
    other = lax.ppermute(mine, "tensor", [(1, 2), (2, 1)])
    done = finish(mine.astype(F32) + other.astype(F32)).astype(BF)
    back_out = lax.ppermute(done, "tensor", [(1, 0), (2, 3)])
    return jnp.where(inner, done, back_out)


def swap(value, bit):
    n = lax.axis_size("dp")
    return lax.ppermute(value, "dp", [(i, i ^ (1 << bit)) for i in range(n)])


def halve(value, bits, order, dtype):
    me = lax.axis_index("dp")
    bits = list(bits)
    for n, bit in enumerate(order):
        at = bits.index(bit)
        high = 1 << at
        view = value.reshape((high, 2, value.shape[0] // (2 * high)) + value.shape[1:])
        b = (me >> bit) & 1
        sent = swap(lax.dynamic_index_in_dim(view, 1 - b, 1, keepdims=False), bit)
        kept = lax.dynamic_index_in_dim(view, b, 1, keepdims=False)
        last = n == len(order) - 1
        value = (kept.astype(F32) + sent.astype(F32)).astype(dtype if last else BF)
        value = value.reshape((-1,) + value.shape[2:])
        bits.remove(bit)
    return value.reshape(value.shape[1:])


def pick(array, b):
    n = lax.axis_size("dp")
    rows, width = array.shape
    return lax.dynamic_index_in_dim(array.reshape(rows, n // 2, 2, width // n), b, 2, keepdims=False).reshape(rows, width // 2)


def weight_grad(left, right):
    n = lax.axis_size("dp")
    bits = n.bit_length() - 1
    b = lax.axis_index("dp") & 1
    sent = swap(dot(pick(left, 1 - b), right, TN).astype(BF), 0)
    kept = (dot(pick(left, b), right, TN) + sent.astype(F32)).astype(BF)
    per = left.shape[1] // n
    kept = kept.reshape(n // 2, per, right.shape[1])
    rest = list(range(bits - 1, 0, -1))
    first = halve(kept[:, : per // 2], rest, rest[::-1], F32)
    second = halve(kept[:, per // 2 :], rest, rest, F32)
    return jnp.concatenate([first, second], axis=0)


def per_device(
    tokens, attn_norm_gain, attn_norm_bias, mlp_norm_gain, mlp_norm_bias, w_qkv, qkv_bias,
    w_out, w_up, up_bias, w_down, out_bias, cotangent,
):
    rows, width = tokens.shape
    tensor_index = lax.axis_index("tensor")
    tensor_size = lax.axis_size("tensor")
    attn_in, mlp_in, mean, inv = norm_forward(tokens, attn_norm_gain, attn_norm_bias, mlp_norm_gain, mlp_norm_bias)
    cosines, sines = rotary_tables(SEQ_LEN)
    projected = dot(attn_in, w_qkv) + qkv_bias
    attended_grad = dot(cotangent, w_out, NT).astype(BF)
    attended, proj_grad, qkv_bias_grad = attention(projected, attended_grad, cosines, sines)

    mids = []
    at = 0
    for size in (512, 512):
        mids.append(middle(mlp_in, cotangent, w_up, up_bias, w_down, at, size))
        at += size

    def piece(at):
        return at // 512, at % 512

    block_out = jnp.zeros((rows, width), BF)
    at = 0
    for size in B_ROWS:
        m, off = piece(at)
        part = branch(mids[m][0], off, attended, at, w_down, w_out, size)
        toks = tokens[at : at + size]
        done = line_sum(part, lambda total, t=toks: t.astype(F32) + total + out_bias)
        block_out = lax.dynamic_update_slice(block_out, done, (at, 0))
        at += size

    input_grad = jnp.zeros((rows, width), F32)
    norm_terms = jnp.zeros((4, width), F32)
    at = 0
    for size in N_ROWS:
        m, off = piece(at)
        part, sums = back(
            mids[m][1], off, proj_grad, at, w_up, w_qkv, tokens, mean, inv, attn_norm_gain, mlp_norm_gain, size
        )
        norm_terms = norm_terms + sums
        sl = slice(at, at + size)
        normed = (tokens[sl].astype(F32) - mean[sl, :1]) * inv[sl, :1]

        def finish(g, normed=normed, scale=inv[sl, :1]):
            g_mean = jnp.mean(g, axis=1, keepdims=True)
            cross = jnp.mean(g * normed, axis=1, keepdims=True)
            return scale * (g - g_mean - normed * cross)

        done = line_sum(part, finish)
        input_grad = lax.dynamic_update_slice(input_grad, cotangent[sl].astype(F32) + done.astype(F32), (at, 0))
        at += size

    hidden = jnp.concatenate([m[0] for m in mids], axis=0)
    up_grad = jnp.concatenate([m[1] for m in mids], axis=0)
    up_bias_grad = sum(m[2] for m in mids)[0]

    grad_w_down = weight_grad(cotangent, hidden).T
    grad_w_out = weight_grad(cotangent, attended).T
    grad_w_up = weight_grad(mlp_in, up_grad)
    grad_w_qkv = weight_grad(attn_in, proj_grad)

    def spread(own):
        return lax.dynamic_update_slice(
            jnp.zeros((own.shape[0] * tensor_size,), F32), own, (tensor_index * own.shape[0],)
        )

    share = rows // tensor_size
    out_bias_part = jnp.sum(
        lax.dynamic_slice_in_dim(cotangent, tensor_index * share, share, 0), axis=0, dtype=F32
    )
    grad_norm_params, grad_qkv_bias, grad_up_bias, grad_out_bias = lax.psum(
        (norm_terms, spread(qkv_bias_grad), spread(up_bias_grad), out_bias_part), ("dp", "tensor")
    )
    return (
        block_out, input_grad, grad_w_qkv, grad_w_out, grad_w_up, grad_w_down,
        grad_norm_params, grad_qkv_bias, grad_up_bias, grad_out_bias,
    )


def solution(mesh):
    placed = (
        P("dp", None), P(), P(), P(), P(), P(None, "tensor"), P("tensor"), P("tensor", None),
        P(None, "tensor"), P("tensor"), P("tensor", None), P(), P("dp", None),
    )
    return jax.shard_map(
        per_device,
        mesh=mesh,
        in_specs=placed,
        out_specs=(
            P("dp", None), P("dp", None), P("dp", "tensor"), P("tensor", "dp"),
            P("dp", "tensor"), P("tensor", "dp"), P(), P(), P(), P(),
        ),
        check_vma=False,
    )
```
